256 devices in a mesh: rows: 4 (over y_lo, core), dp: 64 (over x, y_hi, z).
Axes of the slice: x: 4, y: 4 (y_hi: 2, y_lo: 2; y = y_hi * 2 + y_lo), z: 8, core: 2. Of those that a mesh axis runs over, the one named last changes fastest.
Arguments:
- emb_weight: float32 [64, 6144, 128], P('dp', 'rows'), may hold values from -160 to 160
- emb_grad: bfloat16 [64, 6144, 128], P('dp', 'rows'), may hold values from -6 to 6
- emb_moment: float32 [64, 6144, 128], P('dp', 'rows'), may hold values from -160 to 160
- emb_second: float32 [64, 6144, 128], P('dp', 'rows'), may hold values from 0.1 to 4
- hot_rows: int32 [64, 4, 256], P('dp', 'rows'), may hold values from 0 to 1535
- block_counts: int32 [64, 4], P('dp', 'rows'), may hold values from 1 to 2, as said below
- dense_weight: float32 [512, 256], replicated, may hold values from -8 to 8
- dense_grad: float32 [256, 512, 256], P(('rows', 'dp')), may hold values from -6 to 6
- dense_moment: float32 [512, 256], replicated, may hold values from -900 to 900
- dense_second: float32 [512, 256], replicated, may hold values from 25.6 to 1024
Outputs:
- new_weight: float32 [64, 6144, 128], P('dp', 'rows')
- new_moment: float32 [64, 6144, 128], P('dp', 'rows')
- new_second: float32 [64, 6144, 128], P('dp', 'rows')
- hot_cache: bfloat16 [64, 4, 256, 128], P(None, 'rows')
- fresh_dense: float32 [512, 256], replicated
- fresh_moment: float32 [512, 256], replicated
- fresh_second: float32 [512, 256], replicated
The draws below stay inside these ranges and needn't reach their ends.
Inputs may be any that keep to these rules, and one draw needn't show every extreme that they name: `block_counts`: some table shard has 2 live blocks in every draw. `hot_rows`: entries in dead blocks are ignored.
All inputs are finite; a program needn't handle non-finite values.
Results may differ from the reference program's by a relative error of at most 0.001.
Values may be sent and summed in bfloat16 or wider, within the bound.
No kernel may reach another device: no remote copies, remote signals or barrier semaphores. Data moves between devices by JAX's collectives and lax.ppermute only.
A program may use at most 64 MiB of HBM per device.

```python
import math
import jax
import jax.numpy as jnp
from jax import lax

E = 128
DIN = 512
DOUT = 256
RS = 1536
BLOCK = 128
HB = 2
TABLES = 64
TROWS = 6144
N_ROWS = 4
N_DP = 64


def scaled_field(key, lead, height, width, base_scale, ramped):
    base_key, row_key, col_key = jax.random.split(jax.random.fold_in(key, 11), 3)
    base = jnp.clip(jax.random.normal(base_key, (lead, height, width), jnp.float32), -6.0, 6.0)
    top_ratio = 3.0
    row_scale = jnp.exp(jax.random.uniform(row_key, (lead, height, 1), jnp.float32, math.log(0.3), math.log(3.0)))
    col_scale = jnp.exp(jax.random.uniform(col_key, (lead, 1, width), jnp.float32, math.log(0.3), math.log(3.0)))
    field = base * row_scale * col_scale * base_scale
    if ramped:
        position = jnp.arange(height, dtype=jnp.float32) / (height - 1)
        field = field * jnp.sqrt(1.0 + (top_ratio - 1.0) * position)[None, :, None]
    return field


def draw_emb_weight(key, part):
    return scaled_field(jax.random.fold_in(key, 101), TABLES, TROWS, E, 1.0, True)


def draw_emb_moment(key, part):
    return scaled_field(jax.random.fold_in(key, 202), TABLES, TROWS, E, 1.0, True)


def draw_dense_weight(key, part):
    return scaled_field(jax.random.fold_in(key, 303), 1, DIN, DOUT, DIN ** (-0.5), False)[0]


def draw_dense_moment(key, part):
    return scaled_field(jax.random.fold_in(key, 404), 1, DIN, DOUT, (TROWS // RS * TABLES) ** 0.5, False)[0]


def draw_block_counts(key, part):
    shard_count = TROWS // RS
    count_key, spot_key = jax.random.split(jax.random.fold_in(key, 23))
    counts = jax.random.randint(count_key, (TABLES * shard_count,), 1, HB + 1, dtype=jnp.int32)
    spot_index = jax.random.randint(spot_key, (), 0, TABLES * shard_count, dtype=jnp.int32)
    counts = counts.at[spot_index].set(HB)
    return counts.reshape(TABLES, shard_count)


def set_ends(result, stream_key, least, largest):
    longest = result.shape.index(max(result.shape))
    spots = []
    for shift in (0, 1):
        where = [jax.random.randint(jax.random.fold_in(stream_key, axis), (), 0, length) for axis, length in enumerate(result.shape)]
        where[longest] = (where[longest] + shift) % result.shape[longest]
        spots.append(tuple(where))
    return result.at[spots[0]].set(least).at[spots[1]].set(largest)


def block_levels(key, shape, cuts, least, top_value):
    factor_of = 1.0
    for dim, blocks in cuts:
        heights = jax.random.uniform(jax.random.fold_in(jax.random.fold_in(key, 6), dim), (blocks,), jnp.float32, least / len(cuts), top_value / len(cuts))
        factor_of = factor_of * jnp.repeat(jnp.exp(heights), shape[dim] // blocks).reshape((-1,) + (1,) * (len(shape) - 1 - dim))
    return factor_of


def bell_draw(stream_key, shape, spread, bound, pieces=(), kind=jnp.bfloat16):
    entries = spread * jax.random.normal(stream_key, shape, jnp.float32)
    if pieces:
        entries = entries * block_levels(stream_key, shape, pieces, -0.22, 0.18)
    return jnp.clip(entries, -bound, bound).astype(kind)


def setup_inputs(seed: int = 0) -> dict:
    seeds = jax.random.split(jax.random.key(seed), 11)
    return {
        "emb_weight": draw_emb_weight(jax.random.fold_in(seeds[10], 71), 0),
        "emb_grad": bell_draw(seeds[1], (TABLES, TROWS, E), 1.0, 6.0, ((0, 64), (1, 4))),
        "emb_moment": draw_emb_moment(jax.random.fold_in(seeds[10], 71), 0),
        "emb_second": jnp.clip(jnp.exp(math.log(4.0) - 3.6888794 * jax.random.uniform(seeds[3], (TABLES, TROWS, E), jnp.float32) ** block_levels(seeds[3], (TABLES, TROWS, E), ((0, 64), (1, 4)), -0.2, 0.2)), 0.1, 4.0),
        "hot_rows": set_ends(jax.random.randint(seeds[4], (TABLES, N_ROWS, HB * BLOCK), 0, RS), jax.random.fold_in(seeds[4], 1), 0, RS - 1).astype(jnp.int32),
        "block_counts": draw_block_counts(jax.random.fold_in(seeds[10], 71), 0),
        "dense_weight": draw_dense_weight(jax.random.fold_in(seeds[10], 71), 0),
        "dense_grad": bell_draw(seeds[7], (N_ROWS * N_DP, DIN, DOUT), 1.0, 6.0, ((0, 256),), jnp.float32),
        "dense_moment": draw_dense_moment(jax.random.fold_in(seeds[10], 71), 0),
        "dense_second": jnp.clip(jnp.exp(jax.random.uniform(seeds[9], (DIN, DOUT), jnp.float32, math.log(25.6), math.log(1024.0))), 25.6, 1024.0),
    }


beta_one = 0.9
beta_two = 0.999
first_fix = 1.0 / (1.0 - 0.9 ** 10)
second_fix = 1.0 / (1.0 - 0.999 ** 10)
epsilon = 1e-06
norm_floor = 1e-06
decay_rate = 0.1
learn_rate = 0.05

def moments(weight, gradient, moment, second):
    new_moment = beta_one * moment + (1.0 - beta_one) * gradient
    new_second = beta_two * second + (1.0 - beta_two) * gradient * gradient
    direction = first_fix * new_moment / (jnp.sqrt(second_fix * new_second) + epsilon)
    return (new_moment, new_second, direction)

def trust_step(weight_sq, update_sq):
    return learn_rate * jnp.sqrt(weight_sq + norm_floor) / jnp.sqrt(update_sq + norm_floor)

def one_table(packed):
    weight, gradient, moment, second, row_ids, counts = packed
    new_moment, new_second, direction = moments(weight, gradient.astype(jnp.float32), moment, second)
    update = direction + decay_rate * weight
    step_size = trust_step(jnp.sum(weight * weight), jnp.sum(update * update))
    new_weight = weight - step_size * update
    shards = new_weight.reshape(row_ids.shape[0], -1, new_weight.shape[-1])
    picked = jnp.take_along_axis(shards, row_ids[:, :, None], axis=1)
    live_mask = jnp.arange(row_ids.shape[1], dtype=jnp.int32)[None, :] < BLOCK * counts[:, None]
    cached = jnp.where(live_mask[:, :, None], picked, jnp.zeros_like(picked)).astype(jnp.bfloat16)
    return (new_weight, new_moment, new_second, cached)

def reference(emb_weight, emb_grad, emb_moment, emb_second, hot_rows, block_counts, dense_weight, dense_grad, dense_moment, dense_second):
    tables = lax.map(one_table, (emb_weight, emb_grad, emb_moment, emb_second, hot_rows, block_counts))
    summed_grad = lax.optimization_barrier(jnp.sum(dense_grad, axis=0))
    fresh_moment, fresh_second, heading = moments(dense_weight, summed_grad, dense_moment, dense_second)
    dense_scale = trust_step(jnp.sum(dense_weight * dense_weight), jnp.sum(heading * heading))
    fresh_dense = dense_weight - dense_scale * heading
    return (tables[0], tables[1], tables[2], tables[3], fresh_dense, fresh_moment, fresh_second)
```

```python
import functools

import jax
import jax.numpy as jnp
import numpy as np
from jax import lax
from jax.experimental import pallas as pl
from jax.experimental.pallas import tpu as pltpu
from jax.sharding import PartitionSpec as P


BLOCK = 128
A_ROWS = 144

beta_one = 0.9
beta_two = 0.999
first_fix = 1.0 / (1.0 - 0.9**10)
second_fix = 1.0 / (1.0 - 0.999**10)
epsilon = 1e-06
norm_floor = 1e-06
decay_rate = 0.1
learn_rate = 0.05


def moments(gradient, moment, second):
    new_moment = beta_one * moment + (1.0 - beta_one) * gradient
    new_second = beta_two * second + (1.0 - beta_two) * gradient * gradient
    direction = first_fix * new_moment / (jnp.sqrt(second_fix * new_second) + epsilon)
    return (new_moment, new_second, direction)


def trust_step(weight_sq, update_sq):
    return learn_rate * jnp.sqrt(weight_sq + norm_floor) / jnp.sqrt(update_sq + norm_floor)


def split_dp(i):
    return i // 16, (i // 8) % 2, i % 8


def join_dp(x, yh, z):
    return x * 16 + yh * 8 + z


def z_two(x, yh, z):
    return join_dp(x, yh, (z + 2 + 4 * (z % 2)) % 8)


def z_two_source(x, yh, z):
    return join_dp(x, yh, (z + 6 - 4 * (z % 2)) % 8)


FAR = (
    (lambda x, y, z: join_dp(x, 1 - y, z), lambda x, y, z: join_dp(x, 1 - y, z)),
    (lambda x, y, z: join_dp(x, y, (z + 4) % 8), lambda x, y, z: join_dp(x, y, (z + 4) % 8)),
    (lambda x, y, z: join_dp(x, 1 - y, (z + 4) % 8), lambda x, y, z: join_dp(x, 1 - y, (z + 4) % 8)),
)
ALONG_X = (
    (lambda x, y, z: join_dp((x + 2) % 4, y, z), lambda x, y, z: join_dp((x + 2) % 4, y, z)),
    (lambda x, y, z: join_dp((x + 1) % 4, y, z), lambda x, y, z: join_dp((x + 3) % 4, y, z)),
    (lambda x, y, z: join_dp((x + 3) % 4, y, z), lambda x, y, z: join_dp((x + 1) % 4, y, z)),
)
ALONG_Z = (
    (z_two, z_two_source),
    (lambda x, y, z: join_dp(x, y, (z + 1) % 8), lambda x, y, z: join_dp(x, y, (z + 7) % 8)),
    (lambda x, y, z: join_dp(x, y, (z + 7) % 8), lambda x, y, z: join_dp(x, y, (z + 1) % 8)),
)


def move_dp(value, move):
    return lax.ppermute(value, "dp", [(i, move[0](*split_dp(i))) for i in range(64)])


def move_rows(value, flip):
    return lax.ppermute(value, "rows", [(i, i ^ flip) for i in range(4)])


def move_y(value, flip_low, flip_high):
    pairs = []
    for r in range(4):
        for i in range(64):
            x, y, z = split_dp(i)
            pairs.append((r * 64 + i, (r ^ (2 * flip_low)) * 64 + join_dp(x, y ^ flip_high, z)))
    return lax.ppermute(value, ("rows", "dp"), pairs)


def gathered_ids(ids, moves):
    out = list(ids)
    for _, source in moves:
        for f in ids:
            out.append(functools.partial(lambda f, source, i: f(source(*split_dp(i))), f, source))
    return out


def place_kernel(counts, table_ref, *refs):
    pieces, out_ref, sem = refs[: len(counts)], refs[len(counts)], refs[-1]
    copies = []
    slot = 0
    for (blocks, start, size), piece in zip(counts, pieces):
        for k in range(blocks):
            copies.append(
                pltpu.make_async_copy(
                    piece.at[k], out_ref.at[table_ref[slot], pl.ds(start, size)], sem.at[slot]
                )
            )
            slot += 1
    for copy in copies:
        copy.start()
    for copy in copies:
        copy.wait()


def place(tables, pieces, starts):
    counts = tuple((p.shape[0], s, p.shape[1]) for p, s in zip(pieces, starts))
    total = sum(c[0] for c in counts)
    return pl.pallas_call(
        functools.partial(place_kernel, counts),
        out_shape=jax.ShapeDtypeStruct((64, 256, 128), jnp.bfloat16),
        in_specs=[pl.BlockSpec(memory_space=pltpu.SMEM)]
        + [pl.BlockSpec(memory_space=pl.ANY)] * len(pieces),
        out_specs=pl.BlockSpec(memory_space=pl.ANY),
        scratch_shapes=[pltpu.SemaphoreType.DMA((total,))],
        name="place",
    )(tables, *pieces)


def to_pair(chunk):
    high = lax.reduce_precision(chunk, 8, 7)
    low = lax.reduce_precision(chunk - high, 8, 7)
    both = jnp.concatenate([high[:, :128], high[:, 128:], low[:, :128], low[:, 128:]], axis=0)
    return both.astype(jnp.bfloat16)


def from_pair(both):
    wide = both.astype(jnp.float32)
    return jnp.concatenate([wide[:64] + wide[128:192], wide[64:128] + wide[192:]], axis=1)


def shards(w, g, m, v, hot_rows, block_counts, dense_weight, dense_grad, dense_moment, dense_second):
    rows, dp = lax.axis_index("rows"), lax.axis_index("dp")
    core, yl = rows % 2, rows // 2
    x, yh, z = split_dp(dp)
    w, m, v = w[0], m[0], v[0]

    grad = dense_grad[0]
    kept = lax.dynamic_slice(grad, (core * 256, 0), (256, 256))
    core_part = move_rows(lax.dynamic_slice(grad, ((1 - core) * 256, 0), (256, 256)), 1)

    new_moment, new_second, direction = moments(g[0].astype(jnp.float32), m, v)
    update = direction + decay_rate * w
    weight_sq = jnp.sum(w * w)
    update_sq = jnp.sum(update * update)
    lane = lax.broadcasted_iota(jnp.int32, (8, 128), 1)
    sums = jnp.where(lane == 0, weight_sq, update_sq)
    others = [move_rows(sums, flip) for flip in (1, 2, 3)]
    ids = hot_rows[0, 0]
    picked_weight = jnp.take(w, ids, axis=0, mode="clip")
    picked_update = jnp.take(update, ids, axis=0, mode="clip")
    half = kept + core_part
    quarter = lax.dynamic_slice(half, (yl * 128, 0), (128, 256))
    low_part = move_rows(lax.dynamic_slice(half, ((1 - yl) * 128, 0), (128, 256)), 2)
    sums = (sums + others[0]) + (others[1] + others[2])
    step_size = trust_step(sums[0, 0], sums[0, 1])
    live = lax.broadcasted_iota(jnp.int32, (256, 128), 0) < BLOCK * block_counts[0, 0]
    hot = jnp.where(live, picked_weight - step_size * picked_update, 0.0).astype(jnp.bfloat16)
    quarter = quarter + low_part

    mine = to_pair(lax.dynamic_slice(quarter, (yh * 64, 0), (64, 256)))
    theirs = to_pair(lax.dynamic_slice(quarter, ((1 - yh) * 64, 0), (64, 256)))
    loads = [jnp.concatenate([hot, d], axis=0) for d in (theirs, mine, theirs)]
    got = [move_dp(load, move) for load, move in zip(loads, FAR)]
    d = [from_pair(mine)] + [from_pair(r[256:]) for r in got]
    eighth = (d[0] + d[1]) + (d[2] + d[3])
    blocks = [hot] + [r[:256] for r in got]
    own_a = jnp.stack([b[:A_ROWS] for b in blocks])
    own_b = jnp.stack([b[A_ROWS:] for b in blocks])

    mine = to_pair(eighth)
    b_rows = 256 - A_ROWS
    load_b = jnp.concatenate([own_b.reshape(4 * b_rows, 128), mine], axis=0)
    got_b = [move_dp(load_b, move) for move in ALONG_X]
    got_a = [move_dp(own_a, move) for move in ALONG_Z]
    d = [from_pair(mine)] + [from_pair(r[4 * b_rows :]) for r in got_b]
    eighth = (d[0] + d[1]) + (d[2] + d[3])
    all_a = jnp.concatenate([own_a] + got_a, axis=0)
    all_b = jnp.concatenate([own_b] + [r[: 4 * b_rows].reshape(4, b_rows, 128) for r in got_b], axis=0)

    d = [eighth] + [move_dp(eighth, move) for move in ALONG_Z]
    last_a = [move_dp(all_a, move) for move in ALONG_X]
    last_b = [move_dp(all_b, move) for move in ALONG_Z]
    eighth = (d[0] + d[1]) + (d[2] + d[3])

    e = [eighth] + [move_y(eighth, *flips) for flips in ((0, 1), (1, 0), (1, 1))]
    pairs = [jnp.where(yh == 0, jnp.concatenate([p, q], 0), jnp.concatenate([q, p], 0)) for p, q in ((e[0], e[1]), (e[2], e[3]))]
    half = jnp.where(yl == 0, jnp.concatenate(pairs, 0), jnp.concatenate(pairs[::-1], 0))
    other = move_rows(half, 1)
    summed = jnp.where(core == 0, jnp.concatenate([half, other], 0), jnp.concatenate([other, half], 0))
    fresh_moment, fresh_second, heading = moments(summed, dense_moment, dense_second)
    dense_scale = trust_step(jnp.sum(dense_weight * dense_weight), jnp.sum(heading * heading))
    fresh_dense = dense_weight - dense_scale * heading

    new_weight = w - step_size * update

    ids_one = gathered_ids([lambda i: i], FAR)
    ids_a = gathered_ids(gathered_ids(ids_one, ALONG_Z), ALONG_X)
    ids_b = gathered_ids(gathered_ids(ids_one, ALONG_X), ALONG_Z)
    every = np.array([[f(i) for f in ids_a + ids_b] for i in range(64)], np.int32)
    assert (np.sort(every.reshape(64, 2, 64), axis=2) == np.arange(64)).all()
    tables = lax.dynamic_index_in_dim(jnp.asarray(every), dp, 0, keepdims=False)
    hot_cache = place(tables, [all_a] + last_a + [all_b] + last_b, [0] * 4 + [A_ROWS] * 4)
    return (
        new_weight[None],
        new_moment[None],
        new_second[None],
        hot_cache[:, None],
        fresh_dense,
        fresh_moment,
        fresh_second,
    )


def solution(mesh):
    in_specs = (
        P("dp", "rows", None),
        P("dp", "rows", None),
        P("dp", "rows", None),
        P("dp", "rows", None),
        P("dp", "rows", None),
        P("dp", "rows"),
        P(),
        P(("rows", "dp"), None, None),
        P(),
        P(),
    )
    out_specs = (
        P("dp", "rows", None),
        P("dp", "rows", None),
        P("dp", "rows", None),
        P(None, "rows", None, None),
        P(),
        P(),
        P(),
    )
    return jax.shard_map(shards, mesh=mesh, in_specs=in_specs, out_specs=out_specs, check_vma=False)
```

```python
import functools

import jax
import jax.numpy as jnp
import numpy as np
from jax import lax
from jax.experimental import pallas as pl
from jax.experimental.pallas import tpu as pltpu
from jax.sharding import PartitionSpec as P


BLOCK = 128
A_ROWS = 144

beta_one = 0.9
beta_two = 0.999
first_fix = 1.0 / (1.0 - 0.9**10)
second_fix = 1.0 / (1.0 - 0.999**10)
epsilon = 1e-06
norm_floor = 1e-06
decay_rate = 0.1
learn_rate = 0.05


def moments(gradient, moment, second):
    new_moment = beta_one * moment + (1.0 - beta_one) * gradient
    new_second = beta_two * second + (1.0 - beta_two) * gradient * gradient
    direction = first_fix * new_moment / (jnp.sqrt(second_fix * new_second) + epsilon)
    return (new_moment, new_second, direction)


def trust_step(weight_sq, update_sq):
    return learn_rate * jnp.sqrt(weight_sq + norm_floor) / jnp.sqrt(update_sq + norm_floor)


def split_dp(i):
    return i // 16, (i // 8) % 2, i % 8


def join_dp(x, yh, z):
    return x * 16 + yh * 8 + z


def z_two(x, yh, z):
    return join_dp(x, yh, (z + 2 + 4 * (z % 2)) % 8)


def z_two_source(x, yh, z):
    return join_dp(x, yh, (z + 6 - 4 * (z % 2)) % 8)


FAR = (
    (lambda x, y, z: join_dp(x, 1 - y, z), lambda x, y, z: join_dp(x, 1 - y, z)),
    (lambda x, y, z: join_dp(x, y, (z + 4) % 8), lambda x, y, z: join_dp(x, y, (z + 4) % 8)),
    (lambda x, y, z: join_dp(x, 1 - y, (z + 4) % 8), lambda x, y, z: join_dp(x, 1 - y, (z + 4) % 8)),
)
ALONG_X = (
    (lambda x, y, z: join_dp((x + 2) % 4, y, z), lambda x, y, z: join_dp((x + 2) % 4, y, z)),
    (lambda x, y, z: join_dp((x + 1) % 4, y, z), lambda x, y, z: join_dp((x + 3) % 4, y, z)),
    (lambda x, y, z: join_dp((x + 3) % 4, y, z), lambda x, y, z: join_dp((x + 1) % 4, y, z)),
)
ALONG_Z = (
    (z_two, z_two_source),
    (lambda x, y, z: join_dp(x, y, (z + 1) % 8), lambda x, y, z: join_dp(x, y, (z + 7) % 8)),
    (lambda x, y, z: join_dp(x, y, (z + 7) % 8), lambda x, y, z: join_dp(x, y, (z + 1) % 8)),
)


def move_dp(value, move):
    return lax.ppermute(value, "dp", [(i, move[0](*split_dp(i))) for i in range(64)])


def move_rows(value, flip):
    return lax.ppermute(value, "rows", [(i, i ^ flip) for i in range(4)])


def move_y(value, flip_low, flip_high):
    pairs = []
    for r in range(4):
        for i in range(64):
            x, y, z = split_dp(i)
            pairs.append((r * 64 + i, (r ^ (2 * flip_low)) * 64 + join_dp(x, y ^ flip_high, z)))
    return lax.ppermute(value, ("rows", "dp"), pairs)


def gathered_ids(ids, moves):
    out = list(ids)
    for _, source in moves:
        for f in ids:
            out.append(functools.partial(lambda f, source, i: f(source(*split_dp(i))), f, source))
    return out


def place_kernel(counts, table_ref, *refs):
    pieces, out_ref, sem = refs[: len(counts)], refs[len(counts)], refs[-1]
    copies = []
    slot = 0
    for (blocks, start, size), piece in zip(counts, pieces):
        for k in range(blocks):
            copies.append(
                pltpu.make_async_copy(
                    piece.at[k], out_ref.at[table_ref[slot], pl.ds(start, size)], sem.at[slot]
                )
            )
            slot += 1
    for copy in copies:
        copy.start()
    for copy in copies:
        copy.wait()


def place(tables, pieces, starts):
    counts = tuple((p.shape[0], s, p.shape[1]) for p, s in zip(pieces, starts))
    total = sum(c[0] for c in counts)
    return pl.pallas_call(
        functools.partial(place_kernel, counts),
        out_shape=jax.ShapeDtypeStruct((64, 256, 128), jnp.bfloat16),
        in_specs=[pl.BlockSpec(memory_space=pltpu.SMEM)] + vmem(len(pieces)),
        out_specs=pl.BlockSpec(memory_space=pl.ANY),
        scratch_shapes=[pltpu.SemaphoreType.DMA((total,))],
        name="place",
    )(tables, *pieces)


def vmem(count):
    return [pl.BlockSpec(memory_space=pltpu.VMEM)] * count


def pass_one_kernel(w_ref, g_ref, m_ref, v_ref, nm_ref, nv_ref, up_ref, sums_ref):
    w = w_ref[...]
    nm, nv, direction = moments(g_ref[...].astype(jnp.float32), m_ref[...], v_ref[...])
    update = direction + decay_rate * w
    nm_ref[...] = nm
    nv_ref[...] = nv
    up_ref[...] = update

    @pl.when(pl.program_id(0) == 0)
    def _():
        sums_ref[...] = jnp.zeros_like(sums_ref)

    sums_ref[:8] += jnp.sum((w * w).reshape(-1, 8, 128), axis=0)
    sums_ref[8:] += jnp.sum((update * update).reshape(-1, 8, 128), axis=0)


def pass_one(w, g, m, v):
    rows, step = w.shape[0], 256
    block = pl.BlockSpec((step, 128), lambda i: (i, 0))
    wide = jax.ShapeDtypeStruct(w.shape, jnp.float32)
    return pl.pallas_call(
        pass_one_kernel,
        grid=(rows // step,),
        in_specs=[block] * 4,
        out_specs=[block] * 3 + [pl.BlockSpec((16, 128), lambda i: (0, 0))],
        out_shape=[wide] * 3 + [jax.ShapeDtypeStruct((16, 128), jnp.float32)],
        name="pass_one",
        cost_estimate=pl.CostEstimate(flops=30 * w.size, transcendentals=2 * w.size, bytes_accessed=26 * w.size),
    )(w, g, m, v)


def hot_kernel(count_ref, s0, s1, s2, s3, pw_ref, pu_ref, hot_ref, step_ref):
    total = (s0[...] + s1[...]) + (s2[...] + s3[...])
    weight_sq = jnp.sum(jnp.sum(total[:8], axis=0, keepdims=True), axis=1, keepdims=True)
    update_sq = jnp.sum(jnp.sum(total[8:], axis=0, keepdims=True), axis=1, keepdims=True)
    step = trust_step(weight_sq, update_sq)
    step_ref[...] = jnp.broadcast_to(step, step_ref.shape)
    live = lax.broadcasted_iota(jnp.int32, pw_ref.shape, 0) < BLOCK * count_ref[0, 0]
    fresh = pw_ref[...] - step * pu_ref[...]
    hot_ref[...] = jnp.where(live, fresh, jnp.zeros_like(fresh)).astype(jnp.bfloat16)


def hot_rows_of(counts, sums, picked_weight, picked_update):
    return pl.pallas_call(
        hot_kernel,
        in_specs=[pl.BlockSpec(memory_space=pltpu.SMEM)] + vmem(6),
        out_specs=vmem(2),
        out_shape=[
            jax.ShapeDtypeStruct((256, 128), jnp.bfloat16),
            jax.ShapeDtypeStruct((8, 128), jnp.float32),
        ],
        name="hot",
    )(counts, *sums, picked_weight, picked_update)


def cut_kernel(*refs):
    ins, a_ref, b_ref = refs[:-2], refs[-2], refs[-1]
    for k, ref in enumerate(ins):
        a_ref[k] = ref[:A_ROWS]
        b_ref[k] = ref[A_ROWS:]


def cut(blocks):
    n = len(blocks)
    return pl.pallas_call(
        cut_kernel,
        in_specs=vmem(n),
        out_specs=vmem(2),
        out_shape=[
            jax.ShapeDtypeStruct((n, A_ROWS, 128), jnp.bfloat16),
            jax.ShapeDtypeStruct((n, 256 - A_ROWS, 128), jnp.bfloat16),
        ],
        name="cut",
    )(*blocks)


def pack_kernel(*refs):
    out_ref, at = refs[-1], 0
    for ref in refs[:-1]:
        out_ref[at : at + ref.shape[0]] = ref[...]
        at += ref.shape[0]


def pack(pieces, name):
    n = sum(p.shape[0] for p in pieces)
    return pl.pallas_call(
        pack_kernel,
        in_specs=vmem(len(pieces)),
        out_specs=pl.BlockSpec(memory_space=pltpu.VMEM),
        out_shape=jax.ShapeDtypeStruct((n,) + pieces[0].shape[1:], pieces[0].dtype),
        name=name,
    )(*pieces)


FLIPS = ((0, 0), (0, 1), (1, 0), (1, 1))


def place_of_rows():
    rows, dp = lax.axis_index("rows"), lax.axis_index("dp")
    return rows % 2, rows // 2, (dp // 8) % 2


def flipped(bit, flip):
    return 1 - bit if flip else bit


def eighths_kernel(a_ref, b_ref, *out_refs):
    core, yl, yh = place_of_rows()
    for (low, high), out_ref in zip(FLIPS, out_refs):
        at = core * 256 + flipped(yl, low) * 128 + flipped(yh, high) * 64
        rows = pl.ds(pl.multiple_of(at, 64), 64)
        out_ref[...] = a_ref[rows] + b_ref[rows]


def eighths(own, partner):
    return pl.pallas_call(
        eighths_kernel,
        in_specs=vmem(2),
        out_specs=vmem(4),
        out_shape=[jax.ShapeDtypeStruct((64, 256), jnp.float32)] * 4,
        name="eighths",
    )(own, partner)


def half_kernel(*refs):
    out_ref = refs[-1]
    _, yl, yh = place_of_rows()
    for (low, high), ref in zip(FLIPS, refs[:-1]):
        at = flipped(yl, low) * 128 + flipped(yh, high) * 64
        out_ref[pl.ds(pl.multiple_of(at, 64), 64)] = ref[...]


def half_of(pieces):
    return pl.pallas_call(
        half_kernel,
        in_specs=vmem(4),
        out_specs=pl.BlockSpec(memory_space=pltpu.VMEM),
        out_shape=jax.ShapeDtypeStruct((256, 256), jnp.float32),
        name="half",
    )(*pieces)


def dense_kernel(half_ref, other_ref, w_ref, m_ref, v_ref, out_ref, nm_ref, nv_ref):
    core = lax.axis_index("rows") % 2
    weight_sq = jnp.zeros((8, 256), jnp.float32)
    heading_sq = jnp.zeros((8, 256), jnp.float32)
    for ref, flip in ((half_ref, 0), (other_ref, 1)):
        base = flipped(core, flip) * 256
        for k in range(8):
            rows = pl.ds(pl.multiple_of(base + 32 * k, 32), 32)
            nm, nv, heading = moments(ref[32 * k : 32 * k + 32], m_ref[rows], v_ref[rows])
            nm_ref[rows] = nm
            nv_ref[rows] = nv
            out_ref[rows] = heading
            w = w_ref[rows]
            weight_sq += jnp.sum((w * w).reshape(4, 8, 256), axis=0)
            heading_sq += jnp.sum((heading * heading).reshape(4, 8, 256), axis=0)
    weight_sq = jnp.sum(jnp.sum(weight_sq, axis=0, keepdims=True), axis=1, keepdims=True)
    heading_sq = jnp.sum(jnp.sum(heading_sq, axis=0, keepdims=True), axis=1, keepdims=True)
    scale = trust_step(weight_sq, heading_sq)
    for k in range(16):
        rows = slice(32 * k, 32 * k + 32)
        out_ref[rows] = w_ref[rows] - scale * out_ref[rows]


def dense_update(half, other, w, m, v):
    return pl.pallas_call(
        dense_kernel,
        in_specs=vmem(5),
        out_specs=vmem(3),
        out_shape=[jax.ShapeDtypeStruct((512, 256), jnp.float32)] * 3,
        name="dense",
    )(half, other, w, m, v)


def sum_of(d):
    return (d[0] + d[1]) + (d[2] + d[3])


def shards(w, g, m, v, hot_rows, block_counts, dense_weight, dense_grad, dense_moment, dense_second):
    dp = lax.axis_index("dp")
    w = w[0]

    grad = dense_grad[0]
    partner = move_rows(grad, 1)

    new_moment, new_second, update, sums = pass_one(w, g[0], m[0], v[0])
    sums = [sums] + [move_rows(sums, flip) for flip in (1, 2, 3)]
    ids = hot_rows[0, 0]
    picked_weight = jnp.take(w, ids, axis=0, mode="clip")
    picked_update = jnp.take(update, ids, axis=0, mode="clip")
    hot, step = hot_rows_of(block_counts, sums, picked_weight, picked_update)

    got = [move_dp(hot, move) for move in FAR]
    own_a, own_b = cut([hot] + got)

    got_a = [move_dp(own_a, move) for move in ALONG_Z]
    got_b = [move_dp(own_b, move) for move in ALONG_X]
    all_a = pack([own_a] + got_a, "pack_a")
    all_b = pack([own_b] + got_b, "pack_b")

    last_a = [move_dp(all_a, move) for move in ALONG_X]
    last_b = [move_dp(all_b, move) for move in ALONG_Z]

    d = eighths(grad, partner)
    eighth = sum_of([d[0]] + [move_y(e, *flips) for e, flips in zip(d[1:], FLIPS[1:])])
    eighth = sum_of([eighth] + [move_dp(eighth, move) for move in ALONG_X])
    eighth = eighth + move_dp(eighth, FAR[1])
    eighth = sum_of([eighth] + [move_dp(eighth, move) for move in ALONG_Z])
    half = half_of([eighth] + [move_y(eighth, *flips) for flips in FLIPS[1:]])
    fresh_dense, fresh_moment, fresh_second = dense_update(
        half, move_rows(half, 1), dense_weight, dense_moment, dense_second
    )

    new_weight = w - step[0, 0] * update

    ids_one = gathered_ids([lambda i: i], FAR)
    ids_a = gathered_ids(gathered_ids(ids_one, ALONG_Z), ALONG_X)
    ids_b = gathered_ids(gathered_ids(ids_one, ALONG_X), ALONG_Z)
    every = np.array([[f(i) for f in ids_a + ids_b] for i in range(64)], np.int32)
    assert (np.sort(every.reshape(64, 2, 64), axis=2) == np.arange(64)).all()
    tables = lax.dynamic_index_in_dim(jnp.asarray(every), dp, 0, keepdims=False)
    hot_cache = place(tables, [all_a] + last_a + [all_b] + last_b, [0] * 4 + [A_ROWS] * 4)
    return (
        new_weight[None],
        new_moment[None],
        new_second[None],
        hot_cache[:, None],
        fresh_dense,
        fresh_moment,
        fresh_second,
    )


def solution(mesh):
    in_specs = (
        P("dp", "rows", None),
        P("dp", "rows", None),
        P("dp", "rows", None),
        P("dp", "rows", None),
        P("dp", "rows", None),
        P("dp", "rows"),
        P(),
        P(("rows", "dp"), None, None),
        P(),
        P(),
    )
    out_specs = (
        P("dp", "rows", None),
        P("dp", "rows", None),
        P("dp", "rows", None),
        P(None, "rows", None, None),
        P(),
        P(),
        P(),
    )
    return jax.shard_map(shards, mesh=mesh, in_specs=in_specs, out_specs=out_specs, check_vma=False)
```
